16 devices in a mesh: dp: 2 (over y, z), tp: 8 (over x, core).
Axes of the slice: x: 4, y: 2, z: 1, core: 2. Of those that a mesh axis runs over, the one named last changes fastest.
The devices are a block of a 4x4x8 slice.
Arguments:
- tokens: bfloat16 [6, 4096, 3072], P('dp', 'tp'), parts along dimension 0
- cond_vec: float32 [6, 3072], P('dp'), parts along dimension 0
- txt_len: int32 [6], P('dp'), parts along dimension 0
- grid_hw: int32 [6, 2], P('dp'), parts along dimension 0
- w_mod: bfloat16 [3072, 9216], replicated
- b_mod: float32 [9216], replicated
- w_qkv: bfloat16 [3072, 3, 3072], P(None, None, 'tp')
- b_qkv: float32 [3, 3072], P(None, 'tp')
- q_gain: float32 [128], replicated
- k_gain: float32 [128], replicated
- w_mlp_in: bfloat16 [3072, 12288], P(None, 'tp')
- b_mlp_in: float32 [12288], P('tp')
- w_out_attn: bfloat16 [3072, 3072], P('tp')
- w_out_mlp: bfloat16 [12288, 3072], P('tp')
- b_out: float32 [3072], replicated
Outputs:
- output: bfloat16 [6, 4096, 3072], P('dp', 'tp'), parts along dimension 0
There are 2 independent parts. The reference program is written for one: setup_inputs(seed, part) draws one part's arguments, and reference() takes and returns one part's arrays. A program takes and returns all parts, laid end to end along the dimension named above; an argument that names none is the same for every part.
All inputs are finite; a program needn't handle non-finite values.
Results may differ from the reference program's by a relative error of at most 0.00358401.
Values are sent between devices in bfloat16 or wider.
A program may use at most 768 MiB of HBM per device.

```python
import jax
import jax.numpy as jnp
from jax import lax

BATCH = 3
SEQ = 4096
D = 3072
HEADS = 24
HEAD = 128
FF = 12288
TXT = 256
QBLOCK = 256
GRID_MIN = 16
GRID_MAX = 96
VID = SEQ - TXT
EPS = 1e-6
THETA = 256.0


def setup_inputs(seed: int = 0, part: int = 0) -> dict:
    part_key = jax.random.fold_in(jax.random.key(seed), part)
    act_keys = jax.random.split(part_key, 2)
    int_keys = jax.random.split(jax.random.fold_in(part_key, 1), 3)
    w_keys = jax.random.split(jax.random.key(seed + 1), 11)
    tokens = jax.random.normal(act_keys[0], (BATCH, SEQ, D), jnp.float32).astype(jnp.bfloat16)
    cond_vec = jax.random.normal(act_keys[1], (BATCH, D), jnp.float32)
    sample_idx = jnp.arange(BATCH)
    low_len = jax.random.randint(int_keys[0], (BATCH,), TXT // 8, TXT // 2)
    high_len = jax.random.randint(int_keys[1], (BATCH,), TXT // 2, TXT + 1)
    txt_len = jnp.where(sample_idx % 2 == 0, low_len, high_len)
    txt_len = jnp.where(sample_idx == max(BATCH - 1, 1), TXT, txt_len).astype(jnp.int32)
    grid_hw = jax.random.randint(int_keys[2], (BATCH, 2), GRID_MIN, GRID_MAX + 1)
    first_h = (sample_idx[:, None] == 0) & (jnp.arange(2)[None, :] == 0)
    grid_hw = jnp.where(first_h, GRID_MAX, grid_hw).astype(jnp.int32)
    d_scale = D ** -0.5
    out_scale = (D + FF) ** -0.5
    gate_offset = jnp.where(jnp.arange(3 * D) >= 2 * D, 1.0, 0.0)
    return {
        'tokens': tokens,
        'cond_vec': cond_vec,
        'txt_len': txt_len,
        'grid_hw': grid_hw,
        'w_mod': (jax.random.normal(w_keys[0], (D, 3 * D), jnp.float32) * d_scale).astype(jnp.bfloat16),
        'b_mod': 0.5 * jax.random.normal(w_keys[1], (3 * D,), jnp.float32) + gate_offset,
        'w_qkv': (jax.random.normal(w_keys[2], (D, 3, D), jnp.float32) * d_scale).astype(jnp.bfloat16),
        'b_qkv': 0.3 * jax.random.normal(w_keys[3], (3, D), jnp.float32),
        'q_gain': 1.6 + 0.3 * jax.random.normal(w_keys[4], (HEAD,), jnp.float32),
        'k_gain': 1.6 + 0.3 * jax.random.normal(w_keys[5], (HEAD,), jnp.float32),
        'w_mlp_in': (jax.random.normal(w_keys[6], (D, FF), jnp.float32) * d_scale).astype(jnp.bfloat16),
        'b_mlp_in': 0.3 * jax.random.normal(w_keys[7], (FF,), jnp.float32),
        'w_out_attn': (jax.random.normal(w_keys[8], (D, D), jnp.float32) * out_scale).astype(jnp.bfloat16),
        'w_out_mlp': (jax.random.normal(w_keys[9], (FF, D), jnp.float32) * out_scale).astype(jnp.bfloat16),
        'b_out': 0.3 * jax.random.normal(w_keys[10], (D,), jnp.float32),
    }


def rope_table(grid_hw):
    tok_idx = jnp.arange(SEQ, dtype=jnp.int32)[None, :]
    grid_h = grid_hw[:, 0:1]
    grid_w = grid_hw[:, 1:2]
    t_pos = tok_idx // (grid_h * grid_w)
    h_pos = (tok_idx // grid_w) % grid_h
    w_pos = tok_idx % grid_w
    pair_idx = jnp.arange(HEAD // 2, dtype=jnp.int32)
    axis_sel = (pair_idx >= 8).astype(jnp.int32) + (pair_idx >= 36).astype(jnp.int32)
    within = pair_idx - jnp.where(axis_sel == 0, 0, jnp.where(axis_sel == 1, 8, 36))
    axis_dim = jnp.where(axis_sel == 0, 16.0, 56.0)
    inv_freq = jnp.power(THETA, -2.0 * within.astype(jnp.float32) / axis_dim)
    pos_sel = jnp.where(axis_sel == 0, t_pos[..., None], jnp.where(axis_sel == 1, h_pos[..., None], w_pos[..., None]))
    angles = pos_sel.astype(jnp.float32) * inv_freq
    angles = jnp.where((tok_idx < VID)[..., None], angles, 0.0)
    return jnp.cos(angles), jnp.sin(angles)


def apply_rope(heads_f32, cos_t, sin_t):
    full_shape = heads_f32.shape
    pairs = heads_f32.reshape(full_shape[:-1] + (full_shape[-1] // 2, 2))
    real_part = pairs[..., 0]
    imag_part = pairs[..., 1]
    cos_b = cos_t[:, :, None, :]
    sin_b = sin_t[:, :, None, :]
    rotated = jnp.stack([real_part * cos_b - imag_part * sin_b, real_part * sin_b + imag_part * cos_b], axis=-1)
    return rotated.reshape(full_shape)


def head_rms(heads_f32, gain):
    mean_sq = jnp.mean(heads_f32 * heads_f32, axis=-1, keepdims=True)
    return heads_f32 * lax.rsqrt(mean_sq + EPS) * gain


def attention(q_heads, k_heads, v_heads, tok_valid):
    qk_scale = HEAD ** -0.5
    def one_sample(sample):
        q_one, k_one, v_one, valid_one = sample
        keys_f32 = k_one.astype(jnp.float32)
        vals_f32 = v_one.astype(jnp.float32)
        def one_block(block_id):
            q_blk = lax.dynamic_slice_in_dim(q_one, block_id * QBLOCK, QBLOCK, axis=0).astype(jnp.float32)
            q_valid = lax.dynamic_slice_in_dim(valid_one, block_id * QBLOCK, QBLOCK, axis=0)
            same_seg = q_valid[:, None] == valid_one[None, :]
            scores = jnp.einsum('qhd,khd->hqk', q_blk, keys_f32) * qk_scale
            scores = jnp.where(same_seg[None, :, :], scores, -1e30)
            probs = jax.nn.softmax(scores, axis=-1).astype(jnp.bfloat16).astype(jnp.float32)
            return jnp.einsum('hqk,khd->qhd', probs, vals_f32).astype(jnp.bfloat16)
        blocks = lax.map(one_block, jnp.arange(SEQ // QBLOCK))
        return blocks.reshape(SEQ, HEADS, HEAD)
    return lax.map(one_sample, (q_heads, k_heads, v_heads, tok_valid))


def reference(tokens, cond_vec, txt_len, grid_hw, w_mod, b_mod, w_qkv, b_qkv, q_gain, k_gain, w_mlp_in, b_mlp_in, w_out_attn, w_out_mlp, b_out):
    mod_all = jnp.dot(jax.nn.silu(cond_vec).astype(jnp.bfloat16), w_mod, preferred_element_type=jnp.float32) + b_mod
    shift = mod_all[:, :D]
    scale = mod_all[:, D:2 * D]
    gate = mod_all[:, 2 * D:]
    tok_f32 = tokens.astype(jnp.float32)
    centered = tok_f32 - jnp.mean(tok_f32, axis=-1, keepdims=True)
    variance = jnp.mean(centered * centered, axis=-1, keepdims=True)
    normed = centered * lax.rsqrt(variance + EPS)
    y_mod = (normed * (1.0 + scale[:, None, :]) + shift[:, None, :]).astype(jnp.bfloat16)
    y_rows = y_mod.reshape(BATCH * SEQ, D)
    qkv_f32 = jnp.dot(y_rows, w_qkv.reshape(D, 3 * D), preferred_element_type=jnp.float32).reshape(BATCH, SEQ, 3, D) + b_qkv
    cos_t, sin_t = rope_table(grid_hw)
    head_shape = (BATCH, SEQ, HEADS, HEAD)
    q_heads = apply_rope(head_rms(qkv_f32[:, :, 0].reshape(head_shape), q_gain), cos_t, sin_t).astype(jnp.bfloat16)
    k_heads = apply_rope(head_rms(qkv_f32[:, :, 1].reshape(head_shape), k_gain), cos_t, sin_t).astype(jnp.bfloat16)
    v_heads = qkv_f32[:, :, 2].reshape(head_shape).astype(jnp.bfloat16)
    tok_valid = jnp.arange(SEQ)[None, :] < (VID + txt_len)[:, None]
    attended = attention(q_heads, k_heads, v_heads, tok_valid).reshape(BATCH * SEQ, D)
    mlp_pre = jnp.dot(y_rows, w_mlp_in, preferred_element_type=jnp.float32) + b_mlp_in
    mlp_act = jax.nn.gelu(mlp_pre, approximate=True).astype(jnp.bfloat16)
    projected = jnp.dot(attended, w_out_attn, preferred_element_type=jnp.float32) + jnp.dot(mlp_act, w_out_mlp, preferred_element_type=jnp.float32) + b_out
    result = tok_f32 + gate[:, None, :] * projected.reshape(BATCH, SEQ, D)
    return result.astype(jnp.bfloat16)
```

```python
import functools
import math

import jax
import jax.numpy as jnp
from jax import lax
from jax.experimental import pallas as pl
from jax.experimental.pallas import tpu as pltpu
from jax.sharding import PartitionSpec as P


HEAD = 128
TXT = 256
EPS = 1e-6
THETA = 256.0
NT = (((1,), (1,)), ((), ()))
LOG2E = math.log2(math.e)
SCORE_EXP2 = HEAD ** -0.5 * LOG2E
VMEM = 64 * 1024 * 1024 - 128 * 1024


def qkv_kernel(y_ref, w_ref, b_ref, gain_ref, hot_ref, table_ref, q_ref, k_ref, v_ref, n_ref, *, sub):
    d_local = q_ref.shape[1]
    heads = d_local // HEAD
    stats = [None] * (3 * heads)

    def note(i, val):
        stats[i] = val if stats[i] is None else jnp.maximum(stats[i], val)

    for t in range(y_ref.shape[0] // sub):
        rows = slice(t * sub, (t + 1) * sub)
        cs = jnp.dot(hot_ref[rows, :], table_ref[...], preferred_element_type=jnp.float32)
        cs = cs[:, :2 * HEAD] + (cs[:, 2 * HEAD:4 * HEAD] + cs[:, 4 * HEAD:])
        cos_t, sin_t = cs[:, :HEAD], cs[:, HEAD:]
        hs = sub // 2
        cols = []
        for n in range(0, w_ref.shape[1], 256):
            cols.append(jnp.concatenate([jnp.dot(y_ref[t * sub + i * hs:t * sub + (i + 1) * hs, :], w_ref[:, n:n + 256], preferred_element_type=jnp.float32) for i in range(2)], axis=0))
        z = jnp.concatenate(cols, axis=1) + b_ref[...]
        for part, dst in ((0, q_ref), (1, k_ref)):
            for h in range(heads):
                x = z[:, part * d_local + h * HEAD:part * d_local + (h + 1) * HEAD]
                mean_sq = jnp.mean(x * x, axis=-1, keepdims=True)
                xn = x * lax.rsqrt(mean_sq + EPS) * gain_ref[part:part + 1, :]
                note(part * heads + h, jnp.max(jnp.sum(xn * xn, axis=-1, keepdims=True), axis=0, keepdims=True))
                rot = xn * cos_t + pltpu.roll(xn, HEAD // 2, 1) * sin_t
                dst[rows, h * HEAD:(h + 1) * HEAD] = rot.astype(jnp.bfloat16)
        v = z[:, 2 * d_local:3 * d_local]
        v_ref[rows, :] = v.astype(jnp.bfloat16)
        for h in range(heads):
            note(2 * heads + h, jnp.max(jnp.abs(v[:, h * HEAD:(h + 1) * HEAD]), axis=0, keepdims=True))
    n_ref[...] = jnp.zeros(n_ref.shape, jnp.float32)
    for i in range(3 * heads):
        n_ref[0, i:i + 1, :] = jnp.broadcast_to(stats[i], (1, HEAD))


def qkv_call(y, w, b, gains, hot, table, dl, rb=512, sub=512):
    n, d = y.shape
    d3 = w.shape[1]
    steps = n // rb
    row = lambda c: pl.BlockSpec((rb, c), lambda i: (i, 0))
    whole = lambda *s: pl.BlockSpec(s, lambda i: (0,) * len(s))
    return pl.pallas_call(
        functools.partial(qkv_kernel, sub=sub), grid=(steps,),
        in_specs=[row(d), whole(d, d3), whole(1, d3), whole(2, HEAD), row(hot.shape[1]), whole(*table.shape)],
        out_specs=[row(dl), row(dl), row(dl), pl.BlockSpec((1, 16, HEAD), lambda i: (i, 0, 0))],
        out_shape=[jax.ShapeDtypeStruct((n, dl), jnp.bfloat16)] * 3 + [jax.ShapeDtypeStruct((steps, 16, HEAD), jnp.float32)],
        compiler_params=pltpu.CompilerParams(vmem_limit_bytes=VMEM),
        cost_estimate=pl.CostEstimate(flops=2 * n * d * d3, bytes_accessed=2 * n * d + 2 * n * d3, transcendentals=0),
    )(y, w, b, gains, hot, table)


def attn_kernel(info_ref, q_ref, k_ref, v_ref, o_ref, p_ref, vx_ref, *, sub, bk):
    h = pl.program_id(0)
    i = pl.program_id(1)
    n = k_ref.shape[0]
    bq = q_ref.shape[0]
    vid = n - TXT
    n_valid = info_ref[0]
    fast = info_ref[1 + h] == 1

    def tail_rows(width):
        return lax.broadcasted_iota(jnp.int32, (TXT, width), 0) + vid

    @pl.when(i == 0)
    def _():
        vx_ref[:, :HEAD] = v_ref[...]
        vx_ref[:vid, HEAD:] = jnp.ones((vid, HEAD), jnp.bfloat16)
        keep = jnp.where(tail_rows(HEAD) < n_valid, 1.0, 0.0).astype(jnp.bfloat16)
        vx_ref[vid:, HEAD:] = keep
        vx_ref[vid:, :HEAD] = jnp.where(tail_rows(HEAD) < n_valid, v_ref[vid:, :].astype(jnp.float32), 0.0).astype(jnp.bfloat16)

    @pl.when(fast)
    def _():
        def weighted(t):
            acc = jnp.dot(p_ref[t % 2], vx_ref[...], preferred_element_type=jnp.float32)
            o_ref[t * sub:(t + 1) * sub, :] = (acc[:, :HEAD] / acc[:, HEAD:]).astype(jnp.bfloat16)

        for t in range(bq // sub):
            q = q_ref[t * sub:(t + 1) * sub, :]
            for j in range(n // bk):
                s = lax.dot_general(q, k_ref[j * bk:(j + 1) * bk, :], NT, preferred_element_type=jnp.float32)
                p_ref[t % 2, :, j * bk:(j + 1) * bk] = jnp.exp2(s * SCORE_EXP2).astype(jnp.bfloat16)
            if t > 0:
                weighted(t - 1)
        weighted(bq // sub - 1)

        @pl.when(i == n // bq - 1)
        def _():
            s = lax.dot_general(q_ref[bq - TXT:, :], k_ref[vid:, :], NT, preferred_element_type=jnp.float32)
            p = jnp.exp2(s * SCORE_EXP2).astype(jnp.bfloat16)
            pad = tail_rows(HEAD) >= n_valid
            vp = jnp.where(pad, v_ref[vid:, :].astype(jnp.float32), 0.0).astype(jnp.bfloat16)
            on = jnp.where(pad, 1.0, 0.0).astype(jnp.bfloat16)
            acc = jnp.dot(p, jnp.concatenate([vp, on], axis=1), preferred_element_type=jnp.float32)
            old = o_ref[bq - TXT:, :].astype(jnp.float32)
            o_ref[bq - TXT:, :] = jnp.where(pad, acc[:, :HEAD] / acc[:, HEAD:], old).astype(jnp.bfloat16)

    @pl.when(jnp.logical_not(fast))
    def _():
        bs = 256

        def rows(t, _):
            r0 = pl.multiple_of(t * bs, bs)
            q = q_ref[pl.ds(r0, bs), :]
            q_ok = (lax.broadcasted_iota(jnp.int32, (bs, bs), 0) + (i * bq + r0)) < n_valid

            def keys(j, carry):
                m, acc = carry
                c0 = pl.multiple_of(j * bs, bs)
                s = lax.dot_general(q, k_ref[pl.ds(c0, bs), :], NT, preferred_element_type=jnp.float32) * SCORE_EXP2
                k_ok = (lax.broadcasted_iota(jnp.int32, (bs, bs), 1) + c0) < n_valid
                s = jnp.where(q_ok == k_ok, s, -1e30)
                m_new = jnp.maximum(m, jnp.max(s, axis=1, keepdims=True))
                p = jnp.exp2(s - m_new).astype(jnp.bfloat16)
                vx = jnp.concatenate([v_ref[pl.ds(c0, bs), :], jnp.ones((bs, HEAD), jnp.bfloat16)], axis=1)
                return m_new, acc * jnp.exp2(m - m_new) + jnp.dot(p, vx, preferred_element_type=jnp.float32)

            m0 = jnp.full((bs, 1), -3e38, jnp.float32)
            _, acc = lax.fori_loop(0, n // bs, keys, (m0, jnp.zeros((bs, 2 * HEAD), jnp.float32)))
            o_ref[pl.ds(r0, bs), :] = (acc[:, :HEAD] / acc[:, HEAD:]).astype(jnp.bfloat16)
            return 0

        lax.fori_loop(0, bq // bs, rows, 0)


def attn_call(info, q, k, v, bq=1024, sub=512, bk=1024):
    n, dl = q.shape
    heads = dl // HEAD
    kv = pl.BlockSpec((n, HEAD), lambda h, i, _: (0, h))
    qo = pl.BlockSpec((bq, HEAD), lambda h, i, _: (i, h))
    return pl.pallas_call(
        functools.partial(attn_kernel, sub=sub, bk=bk),
        grid_spec=pltpu.PrefetchScalarGridSpec(
            num_scalar_prefetch=1, grid=(heads, n // bq), in_specs=[qo, kv, kv], out_specs=qo,
            scratch_shapes=[pltpu.VMEM((2, sub, n), jnp.bfloat16), pltpu.VMEM((n, 2 * HEAD), jnp.bfloat16)]),
        out_shape=jax.ShapeDtypeStruct((n, dl), jnp.bfloat16),
        compiler_params=pltpu.CompilerParams(vmem_limit_bytes=VMEM),
        cost_estimate=pl.CostEstimate(flops=8 * n * n * dl, bytes_accessed=8 * n * dl, transcendentals=n * n * heads),
    )(info, q, k, v)


def mlp_kernel(*refs, ts, steps, n_stacks, first, proj, final, aliased, nw):
    refs = list(refs)
    take = lambda k: [refs.pop(0) for _ in range(k)]
    n = len(ts)
    y_hbm = take(n if steps else 0)
    acc_hbm = take(0 if first else n)
    packs, bias = take(n_stacks), take(n_stacks)
    att_hbm = dict(zip(proj, take(len(proj))))
    oa_hbm, = take(1) if proj else (None,)
    tok_hbm, gate_ref, bout_ref = take(3) if final else (None,) * 3
    take(int(aliased))
    accs_out = [t for t in ts if t not in final]
    out_acc = dict(zip(accs_out, take(len(accs_out))))
    out_hbm, = take(1) if final else (None,)
    y_v, acc_v, w_v, u_v, h_v, bias_v, att_v, tok_v, y_sem, acc_sem, w_sem, out_sem, att_sem, tok_sem = refs
    tb, d_model = acc_v.shape[1:]
    _, _, group, width, _ = w_v.shape
    kdim = group * width
    n_steps = len(steps)
    chunk = 2 * kdim
    n_proj = d_model // chunk if proj else 0

    y_copy = lambda i: pltpu.make_async_copy(y_hbm[i], y_v.at[i], y_sem.at[i])
    acc_copy = lambda i: pltpu.make_async_copy(acc_hbm[i], acc_v.at[i], acc_sem.at[i])
    acc_store = lambda i: pltpu.make_async_copy(acc_v.at[i], out_acc[ts[i]], out_sem.at[i])
    out_rows = lambda i: pl.ds(ts[i] * tb, tb)
    tok_copy = lambda i: pltpu.make_async_copy(tok_hbm.at[out_rows(i), :], tok_v.at[final.index(ts[i])], tok_sem.at[final.index(ts[i])])
    out_store = lambda i: pltpu.make_async_copy(tok_v.at[final.index(ts[i])], out_hbm.at[out_rows(i), :], out_sem.at[i])

    def att_copies(j):
        att = att_hbm[proj[j]]
        w = att.shape[2]
        return [pltpu.make_async_copy(att.at[k], att_v.at[j, :, pl.ds(k * w, w)], att_sem.at[j, k]) for k in range(att.shape[0])]

    def weight_copies(s, slot, kind):
        if s >= n_steps:
            return [pltpu.make_async_copy(oa_hbm.at[s - n_steps, kind], w_v.at[slot, kind], w_sem.at[slot, kind, 0])]
        out, at = [], 0
        for k, (i, shard, b0, nb) in enumerate(steps[s]):
            out.append(pltpu.make_async_copy(packs[i].at[shard, kind, pl.ds(b0, nb)], w_v.at[slot, kind, pl.ds(at, nb)], w_sem.at[slot, kind, k]))
            at += nb
        return out

    def start_weights(s):
        for kind in range(2):
            for c in weight_copies(s, s % 2, kind):
                c.start()

    def arrive(s, slot):
        for kind in range(2):
            for c in weight_copies(s, slot, kind):
                c.wait()

    def follow(s, total, low):
        for k in range(low, total):
            @pl.when(s + 1 == k)
            def _():
                start_weights(k)

    def up(k, s, slot):
        t = lax.rem(k, n)
        for p in range(0, group, 2):
            w = w_v[slot, 0, p:p + 2].reshape(2 * width, d_model)
            at = slice(p * width, (p + 2) * width)
            u_v[:, at] = lax.dot_general(y_v[t], w, NT, preferred_element_type=jnp.float32) + bias_v[s, :, at]

    def act():
        h_v[...] = jax.nn.gelu(u_v[...], approximate=True).astype(jnp.bfloat16)

    def down(k, slot):
        t = lax.rem(k, n)
        for c in range(0, d_model, nw):
            w2 = w_v[slot, 1, :, :, c:c + nw].reshape(kdim, nw)
            old = acc_v[t, :, c:c + nw]
            if first:
                old = jnp.where(k < n, 0.0, old)
            acc_v[t, :, c:c + nw] = old + jnp.dot(h_v[...], w2, preferred_element_type=jnp.float32)

    total = n_steps + n_proj
    if n_steps:
        y_copy(0).start()
    start_weights(0)
    for s, parts in enumerate(steps):
        at = 0
        for i, shard, b0, nb in parts:
            for b in range(b0, b0 + nb):
                bias_v[s, :, at * width:(at + 1) * width] = bias[i][shard, b:b + 1, :]
                at += 1
    if n_steps:
        y_copy(0).wait()
        arrive(0, 0)
        for i in range(1, n):
            y_copy(i).start()
    if not first:
        for i in range(n):
            acc_copy(i).start()
    for j in range(len(proj)):
        for c in att_copies(j):
            c.start()
    for t in final:
        tok_copy(ts.index(t)).start()
    if n_steps:
        up(0, 0, 0)
        last = n * n_steps - 1

        def trip(k, _):
            s = lax.div(k, n)
            before = lax.div(k - 1, n)
            for i in range(1, n):
                @pl.when(k == i)
                def _():
                    y_copy(i).wait()
            if not first:
                for i in range(n):
                    @pl.when(k - 1 == i)
                    def _():
                        acc_copy(i).wait()
            if n_steps > 1:
                @pl.when((lax.rem(k, n) == 0) & (k > 0))
                def _():
                    arrive(0, lax.rem(s, 2))
            if total > 1:
                @pl.when(lax.rem(k, n) == 1)
                def _():
                    follow(s, total, 1)
            if not proj:
                for i in range(n - 2):
                    @pl.when(k - 2 - (last + 1 - n) == i)
                    def _():
                        acc_store(i).start()
            act()
            up(k, s, lax.rem(s, 2))
            down(k - 1, lax.rem(before, 2))
            return 0

        lax.fori_loop(1, last + 1, trip, 0)
        if not proj and n > 1:
            acc_store(n - 2).start()
        act()
        if not first and n_steps == 1:
            acc_copy(n - 1).wait()
        down(last, (n_steps - 1) % 2)
        if not proj:
            acc_store(n - 1).start()
    elif not first:
        for i in range(n):
            acc_copy(i).wait()
    if proj:
        for i, t in enumerate(ts):
            if t not in proj:
                acc_store(i).start()
        for j in range(len(proj)):
            for c in att_copies(j):
                c.wait()
        base = ts.index(proj[0])

        def turn(k, _, closing=False):
            c = lax.div(k, len(proj)) if not closing else n_proj - 1
            j = lax.rem(k, len(proj)) if not closing else k
            slot = lax.rem(n_steps + c, 2)
            if not closing:
                @pl.when(j == 0)
                def _():
                    arrive(n_steps, slot)
                    follow(n_steps + c, total, n_steps + 1)
            elif j == 0:
                arrive(n_steps, slot)
            t = proj[j] if closing else None
            last = closing and t in final
            if last:
                tok_copy(base + j).wait()
            at = c * chunk if closing else pl.multiple_of(c * chunk, chunk)
            h = att_v[j, :, pl.ds(at, chunk)]
            for e in range(0, d_model, nw):
                w2 = w_v[slot, :, :, :, e:e + nw].reshape(chunk, nw)
                part = acc_v[base + j, :, e:e + nw] + jnp.dot(h, w2, preferred_element_type=jnp.float32)
                if last:
                    f = final.index(t)
                    res = tok_v[f, :, e:e + nw].astype(jnp.float32) + gate_ref[t:t + 1, e:e + nw] * (part + bout_ref[:, e:e + nw])
                    tok_v[f, :, e:e + nw] = res.astype(jnp.bfloat16)
                else:
                    acc_v[base + j, :, e:e + nw] = part
            if closing:
                (out_store if last else acc_store)(base + j).start()
            return 0

        lax.fori_loop(0, (n_proj - 1) * len(proj), turn, 0)
        for j in range(len(proj)):
            turn(j, 0, closing=True)
    for i, t in enumerate(ts):
        (out_store if t in final else acc_store)(i).wait()


def mlp_call(ts, y, acc, stacks, steps, proj=(), att=(), w_oa=None, final=(), tail=None, group=4, nw=512):
    tb, d = (y or acc)[0].shape
    n = len(ts)
    first = acc is None
    width = 128
    hbm = pl.BlockSpec(memory_space=pl.ANY)
    vm = pl.BlockSpec(memory_space=pltpu.VMEM)
    args, specs = [], []

    def add(spec, *xs):
        args.extend(xs)
        specs.extend([spec] * len(xs))

    if steps:
        add(hbm, *y)
    if not first:
        add(hbm, *acc)
    add(hbm, *[s[0] for s in stacks])
    add(vm, *[s[1] for s in stacks])
    add(hbm, *att)
    if proj:
        add(hbm, w_oa.reshape(d // (2 * group * width), 2, group, width, d))
    alias = {}
    n_acc = n - len(final)
    outs = [jax.ShapeDtypeStruct((tb, d), jnp.float32)] * n_acc
    if final:
        tokens, gate, b_out, out = tail
        add(hbm, tokens)
        add(vm, gate, b_out)
        if out is not None:
            add(hbm, out)
            alias = {len(args) - 1: n_acc}
        outs.append(jax.ShapeDtypeStruct(tokens.shape, tokens.dtype))
    n_steps = len(steps)
    n_par = max(1, len(proj))
    has = lambda c, *s: s if c else (8, 128)
    scratch = [
        pltpu.VMEM(has(n_steps, n, tb, d), jnp.bfloat16), pltpu.VMEM((n, tb, d), jnp.float32),
        pltpu.VMEM((2, 2, group, width, d), jnp.bfloat16),
        pltpu.VMEM(has(n_steps, tb, group * width), jnp.float32), pltpu.VMEM(has(n_steps, tb, group * width), jnp.bfloat16),
        pltpu.VMEM((max(1, n_steps), 1, group * width), jnp.float32),
        pltpu.VMEM(has(proj, n_par, tb, d), jnp.bfloat16), pltpu.VMEM(has(final, max(1, len(final)), tb, d), jnp.bfloat16),
        pltpu.SemaphoreType.DMA((n,)), pltpu.SemaphoreType.DMA((n,)), pltpu.SemaphoreType.DMA((2, 2, 2)), pltpu.SemaphoreType.DMA((n,)),
        pltpu.SemaphoreType.DMA((n_par, 8)), pltpu.SemaphoreType.DMA((max(1, len(final)),))]
    cols = n_steps * group * width
    rows = n * tb
    res = pl.pallas_call(
        functools.partial(mlp_kernel, ts=tuple(ts), steps=steps, n_stacks=len(stacks), first=first, proj=tuple(proj), final=tuple(final), aliased=bool(alias), nw=nw),
        in_specs=specs, out_specs=[hbm] * len(outs), out_shape=outs, input_output_aliases=alias, scratch_shapes=scratch,
        compiler_params=pltpu.CompilerParams(vmem_limit_bytes=VMEM),
        cost_estimate=pl.CostEstimate(flops=4 * rows * d * cols + 2 * len(proj) * tb * d * d, bytes_accessed=4 * d * cols + 10 * rows * d, transcendentals=rows * cols),
    )(*args)
    return (list(res[:n_acc]), res[n_acc]) if final else (list(res), None)


def pick_kernel(where_ref, src_hbm, dst_hbm, buf, in_sem, out_sem):
    n = dst_hbm.shape[0]
    todo = [(i, j) for i in range(n) for j in range(dst_hbm.shape[1])]
    load = lambda i, j: pltpu.make_async_copy(src_hbm.at[where_ref[i], j], buf.at[i, j], in_sem.at[i, j])
    store = lambda i, j: pltpu.make_async_copy(buf.at[i, j], dst_hbm.at[i, j], out_sem.at[i, j])
    for ij in todo:
        load(*ij).start()
    for ij in todo:
        load(*ij).wait()
        store(*ij).start()
    for ij in todo:
        store(*ij).wait()


def pick_call(where, a):
    shape = (where.shape[0],) + a.shape[1:]
    hbm = pl.BlockSpec(memory_space=pl.ANY)
    return pl.pallas_call(
        pick_kernel,
        grid_spec=pltpu.PrefetchScalarGridSpec(
            num_scalar_prefetch=1, grid=(1,), in_specs=[hbm], out_specs=hbm,
            scratch_shapes=[pltpu.VMEM(shape, a.dtype), pltpu.SemaphoreType.DMA(shape[:2]), pltpu.SemaphoreType.DMA(shape[:2])]),
        out_shape=jax.ShapeDtypeStruct(shape, a.dtype),
        compiler_params=pltpu.CompilerParams(vmem_limit_bytes=VMEM),
        cost_estimate=pl.CostEstimate(flops=4 * math.prod(shape), bytes_accessed=4 * math.prod(shape), transcendentals=0),
    )(where, a)


def pack_kernel(first_ref, in_ref, out_ref, o_ref):
    o_ref[0, 0] = in_ref[...].T
    o_ref[1, 0] = out_ref[...]


def pack_call(first, count, w_in, w_out, width):
    d = w_in.shape[0]
    return pl.pallas_call(
        pack_kernel,
        grid_spec=pltpu.PrefetchScalarGridSpec(
            num_scalar_prefetch=1, grid=(count,),
            in_specs=[pl.BlockSpec((d, width), lambda i, f: (0, f[0] + i)), pl.BlockSpec((width, d), lambda i, f: (f[0] + i, 0))],
            out_specs=pl.BlockSpec((2, 1, width, d), lambda i, f: (0, i, 0, 0))),
        out_shape=jax.ShapeDtypeStruct((2, count, width, d), w_in.dtype),
        cost_estimate=pl.CostEstimate(flops=4 * count * width * d, bytes_accessed=8 * count * width * d, transcendentals=0),
    )(first[None], w_in, w_out)


def mod_kernel(me_ref, c_ref, w_ref, o_ref):
    @pl.when(pl.program_id(0) == 0)
    def _():
        o_ref[...] = jnp.zeros(o_ref.shape, jnp.float32)

    o_ref[...] += jnp.dot(c_ref[...], w_ref[...], preferred_element_type=jnp.float32)


def mod_call(me, cond, w, cols, kb=768):
    b, d = cond.shape
    return pl.pallas_call(
        mod_kernel,
        grid_spec=pltpu.PrefetchScalarGridSpec(
            num_scalar_prefetch=1, grid=(d // kb,),
            in_specs=[pl.BlockSpec((b, kb), lambda i, m: (0, i)), pl.BlockSpec((kb, cols), lambda i, m: (i, m[0]))],
            out_specs=pl.BlockSpec((b, cols), lambda i, m: (0, 0))),
        out_shape=jax.ShapeDtypeStruct((b, cols), jnp.float32),
        cost_estimate=pl.CostEstimate(flops=2 * b * d * cols, bytes_accessed=2 * d * cols, transcendentals=0),
    )(me[None], cond, w)


def order_kernel(w_ref, hot_ref, o_ref):
    d_local = w_ref.shape[2]
    for c in range(2):
        for h in range(d_local // HEAD):
            at = slice(h * HEAD, (h + 1) * HEAD)
            o_ref[:, c * d_local + h * HEAD:c * d_local + (h + 1) * HEAD] = jnp.dot(
                w_ref[c, :, at], hot_ref[...], preferred_element_type=jnp.float32).astype(o_ref.dtype)
    o_ref[:, 2 * d_local:3 * d_local] = w_ref[2]
    o_ref[:, 3 * d_local:] = jnp.zeros((o_ref.shape[0], o_ref.shape[1] - 3 * d_local), o_ref.dtype)


def order_call(w, hot, rb=512):
    _, d, d_local = w.shape
    cols = -(-3 * d_local // 256) * 256
    return pl.pallas_call(
        order_kernel, grid=(d // rb,),
        in_specs=[pl.BlockSpec((3, rb, d_local), lambda i: (0, i, 0)), pl.BlockSpec((HEAD, HEAD), lambda i: (0, 0))],
        out_specs=pl.BlockSpec((rb, cols), lambda i: (i, 0)),
        out_shape=jax.ShapeDtypeStruct((d, cols), w.dtype),
        cost_estimate=pl.CostEstimate(flops=4 * d * d_local * HEAD, bytes_accessed=12 * d * d_local, transcendentals=0),
    )(w, hot)


def rope_rows(grid_hw, seq_len, sizes):
    tok_idx = jnp.arange(seq_len, dtype=jnp.int32)
    grid_h, grid_w = grid_hw[0], grid_hw[1]
    video = (tok_idx < seq_len - TXT).astype(jnp.int32)
    pos = (tok_idx // (grid_h * grid_w), (tok_idx // grid_w) % grid_h, tok_idx % grid_w)
    lane = jnp.arange(2 * HEAD, dtype=jnp.int32)[None, :]
    hit, start = None, 0
    for p, size in zip(pos, sizes):
        here = lane == (p * video + start)[:, None]
        hit = here if hit is None else hit | here
        start += size
    return hit.astype(jnp.bfloat16)


def rope_table(sizes):
    pair_idx = jnp.arange(HEAD // 2, dtype=jnp.int32)
    axis_sel = (pair_idx >= 8).astype(jnp.int32) + (pair_idx >= 36).astype(jnp.int32)
    within = pair_idx - jnp.where(axis_sel == 0, 0, jnp.where(axis_sel == 1, 8, 36))
    inv_freq = jnp.power(THETA, -2.0 * within.astype(jnp.float32) / jnp.where(axis_sel == 0, 16.0, 56.0))
    row = jnp.arange(2 * HEAD, dtype=jnp.int32)[:, None]
    start, table = 0, jnp.zeros((2 * HEAD, 2 * HEAD), jnp.float32)
    for axis, size in enumerate(sizes):
        angles = (row - start).astype(jnp.float32) * inv_freq
        cos_t, sin_t = jnp.cos(angles), jnp.sin(angles)
        live = (row >= start) & (row < start + size) & (jnp.tile(axis_sel, 4)[None, :] == axis)
        table = jnp.where(live, jnp.concatenate([cos_t, cos_t, -sin_t, sin_t], axis=1), table)
        start += size
    top = table.astype(jnp.bfloat16)
    rest = table - top.astype(jnp.float32)
    mid = rest.astype(jnp.bfloat16)
    low = (rest - mid.astype(jnp.float32)).astype(jnp.bfloat16)
    return jnp.concatenate([top, mid, low], axis=1)


def modulated_norm(tokens, shift, scale):
    tok_f32 = tokens.astype(jnp.float32)
    centered = tok_f32 - jnp.mean(tok_f32, axis=-1, keepdims=True)
    variance = jnp.mean(centered * centered, axis=-1, keepdims=True)
    normed = centered * lax.rsqrt(variance + EPS)
    return (normed * (1.0 + scale) + shift).astype(jnp.bfloat16)


def split_pairs(x):
    s = x.shape
    return jnp.swapaxes(x.reshape(s[:-1] + (s[-1] // HEAD, HEAD // 2, 2)), -1, -2).reshape(s)


def solution(mesh):
    n_tp, n_dp = mesh.shape['tp'], mesh.shape['dp']
    n_x = n_tp // 2
    twin = [(i, i ^ 1) for i in range(n_dp)]
    core = [(i, i ^ 1) for i in range(n_tp)]

    def block_step(tokens, cond_vec, txt_len, grid_hw, w_mod, b_mod, w_qkv, b_qkv, q_gain, k_gain, w_mlp_in, b_mlp_in, w_out_attn, w_out_mlp, b_out):
        batch, rows, d_model = tokens.shape
        seq = rows * n_tp
        d_local = w_qkv.shape[2]
        heads = d_local // HEAD
        width = 128
        n_blk = w_mlp_in.shape[1] // width
        half = n_blk // 2
        side = lax.axis_index('dp') % 2
        me = lax.axis_index('tp')
        cpos, xpos = me % 2, me // 2

        def after(x, *deps):
            return lax.optimization_barrier((x,) + deps)[0]

        def gather(a, tiled=False):
            return lax.all_gather(a, 'tp', axis=0, tiled=tiled)

        def gather_small(a):
            a, step = a[None], 1
            while step < n_tp:
                b = lax.ppermute(a, 'tp', [(i, i ^ step) for i in range(n_tp)])
                a = jnp.where((me // step) % 2 == 0, jnp.concatenate([a, b]), jnp.concatenate([b, a]))
                step *= 2
            return a

        swap = lambda a: lax.ppermute(a, 'tp', core)
        cross = lambda a: lax.ppermute(a, 'dp', twin)
        mine = side * half
        theirs = half - mine
        chunks = ((0, 2), (2, 2), (4, 2))
        pack = lambda first, count, *deps: pack_call(after(first, *deps), count, w_mlp_in, w_out_mlp, width)
        packs = [pack(mine, chunks[0][1])]

        n_mod = w_mod.shape[1] // n_tp
        mod_part = mod_call(after(me, packs[0]), jax.nn.silu(cond_vec).astype(jnp.bfloat16), w_mod, n_mod)
        small = gather_small(jnp.concatenate([mod_part.reshape(-1), b_mlp_in]))
        own_pack = pack(theirs, half, mod_part)[None]
        mate_pack = swap(own_pack)
        for b0, nb in chunks[1:]:
            packs.append(pack(mine + b0, nb, own_pack))
        mod_all = jnp.swapaxes(small[:, :batch * n_mod].reshape(n_tp, batch, n_mod), 0, 1).reshape(batch, -1) + b_mod
        shift, scale, gate = mod_all[:, :d_model], mod_all[:, d_model:2 * d_model], mod_all[:, 2 * d_model:]
        bias = small[:, batch * n_mod:].reshape(n_tp, n_blk, width)
        bias_g = lax.dynamic_slice_in_dim(bias, mine, half, 1)
        bias_n = lax.dynamic_slice_in_dim(bias, theirs, half, 1)
        y_own = [modulated_norm(tokens[s], shift[s], scale[s]) for s in range(batch)]
        y_full = [gather(y_own[s], tiled=True) for s in range(batch)]
        l_pack = [gather(packs[i]) for i in range(len(chunks))]
        w_oa = gather(w_out_attn, tiled=True)

        far_ids = jnp.stack([2 * ((xpos + j) % n_x) + cpos for j in range(1, n_x)])
        near_ids = [2 * ((xpos + j) % n_x) + 1 - cpos for j in range(1, n_x)]
        perm = jnp.arange(HEAD)
        perm = (perm % (HEAD // 2)) * 2 + perm // (HEAD // 2)
        one_hot = (jnp.arange(HEAD)[:, None] == perm[None, :]).astype(jnp.bfloat16)
        w_all = order_call(jnp.swapaxes(w_qkv, 0, 1), one_hot)
        b_all = jnp.concatenate([split_pairs(b_qkv[:2]).reshape(-1), b_qkv[2], jnp.zeros((w_all.shape[1] - 3 * d_local,), jnp.float32)])[None]
        gains = split_pairs(jnp.stack([q_gain, k_gain]))
        sizes = (16, 96, 96)
        table = rope_table(sizes)
        hots = [rope_rows(grid_hw[s], seq, sizes) for s in range(batch)]

        own = (own_pack, lax.dynamic_index_in_dim(bias_n, me, 0))
        mate = (mate_pack, lax.dynamic_index_in_dim(bias_n, me ^ 1, 0))
        left, far, near, qkv, att, spread = {}, {}, {}, {}, {}, {}
        state = {'last': None, 'acc': None, 'out': None}

        def turn(x):
            return x if state['last'] is None else after(x, state['last'])

        def do_send(i):
            b0, nb = chunks[i]
            left[i] = (l_pack[i], bias_g[:, b0:b0 + nb])
            state['last'] = pick_call(far_ids, turn(l_pack[i]))
            far[i] = (cross(state['last']), jnp.stack([bias_n[2 * ((xpos + j) % n_x) + cpos, b0:b0 + nb] for j in range(1, n_x)]))

        def do_relay(i):
            b0, nb = chunks[i]
            near[i] = (swap(turn(far[i][0])), jnp.stack([bias_n[j, b0:b0 + nb] for j in near_ids]))

        def do_qkv(s):
            qkv[s] = qkv_call(turn(y_full[s]), w_all, b_all, gains, hots[s], table, d_local)
            state['last'] = qkv[s][0]

        def do_attend(s):
            q, k, v, stats = qkv[s]
            top = jnp.max(stats, axis=(0, 2))
            bound = jnp.sqrt(top[:heads] * top[heads:2 * heads]) * (SCORE_EXP2 * 1.02) + 1.0
            v_top = top[2 * heads:3 * heads]
            fast = (bound < 100.0) & (v_top * jnp.exp2(bound) < 2.0 ** 110)
            info = jnp.concatenate([(seq - TXT + txt_len[s])[None], fast.astype(jnp.int32)])
            att[s] = attn_call(info, turn(q), k, v)
            state['last'] = att[s]
            spread[s] = lax.all_to_all(att[s].reshape(n_tp, rows, d_local), 'tp', 0, 0, tiled=False)

        def do_mlp(names, proj=(), final=(), ts=tuple(range(batch))):
            stacks, flat = [], []
            for name in names:
                i = int(name[1:] or 0)
                for stack in {'O': (own, mate), 'L': (left.get(i),), 'D': (far.get(i), near.get(i))}[name[0]]:
                    stacks.append(stack)
                    n_shards, _, nb = stack[0].shape[:3]
                    flat += [(len(stacks) - 1, j, b, 2) for j in range(n_shards) for b in range(0, nb, 2)]
            steps = [flat[i:i + 2] for i in range(0, len(flat), 2)]
            y = [y_own[t] for t in ts]
            acc = state['acc'] and [state['acc'][t] for t in ts]
            if acc:
                acc[0] = turn(acc[0])
            elif steps:
                y[0] = turn(y[0])
            tail = (tokens.reshape(batch * rows, d_model), gate, b_out[None], state['out'])
            accs, out = mlp_call(ts, y, acc, stacks, steps, proj=proj, att=[spread[t] for t in proj], w_oa=w_oa, final=final, tail=tail)
            left_over = [t for t in ts if t not in final]
            state['acc'] = {**(state['acc'] or {}), **dict(zip(left_over, accs))}
            if out is not None:
                state['out'] = out
            state['last'] = (accs + [out])[0]

        do_mlp(['O'])
        state['last'] = after(state['last'], w_all, *hots)
        do_send(0)
        do_mlp(['L0'])
        do_qkv(0)
        do_attend(0)
        do_relay(0)
        do_send(1)
        do_mlp(['L1'])
        do_send(2)
        do_mlp(['D0', 'L2'])
        do_relay(1)
        do_qkv(1)
        do_attend(1)
        do_mlp(['D1'])
        do_qkv(2)
        do_relay(2)
        do_attend(2)
        do_mlp(['D2'], proj=(0, 1), final=(0, 1))
        do_mlp([], proj=(2,), final=(2,), ts=(2,))
        return state['out'].reshape(batch, rows, d_model)

    in_specs = (P('dp', 'tp', None), P('dp', None), P('dp'), P('dp', None), P(None, None), P(None), P(None, None, 'tp'), P(None, 'tp'), P(None), P(None), P(None, 'tp'), P('tp'), P('tp', None), P('tp', None), P(None))
    return jax.shard_map(block_step, mesh=mesh, in_specs=in_specs, out_specs=P('dp', 'tp', None), check_vma=False)
```

```python
import functools
import math

import jax
import jax.numpy as jnp
from jax import lax
from jax.experimental import pallas as pl
from jax.experimental.pallas import tpu as pltpu
from jax.sharding import PartitionSpec as P


HEAD = 128
TXT = 256
EPS = 1e-6
THETA = 256.0
NT = (((1,), (1,)), ((), ()))
LOG2E = math.log2(math.e)
GELU_0 = math.sqrt(2.0 / math.pi)
GELU_1 = 0.044715 * GELU_0
SCORE_EXP2 = HEAD ** -0.5 * LOG2E
VMEM = 64 * 1024 * 1024 - 128 * 1024


def qkv_kernel(y_ref, w_ref, b_ref, gain_ref, hot_ref, table_ref, q_ref, k_ref, v_ref, n_ref, *, sub):
    d_local = q_ref.shape[1]
    heads = d_local // HEAD
    stats = [None] * (3 * heads)

    def note(i, val):
        stats[i] = val if stats[i] is None else jnp.maximum(stats[i], val)

    for t in range(y_ref.shape[0] // sub):
        rows = slice(t * sub, (t + 1) * sub)
        cs = jnp.dot(hot_ref[rows, :], table_ref[...], preferred_element_type=jnp.float32)
        cs = cs[:, :2 * HEAD] + (cs[:, 2 * HEAD:4 * HEAD] + cs[:, 4 * HEAD:])
        cos_t, sin_t = cs[:, :HEAD], cs[:, HEAD:]
        hs = sub // 2
        cols = []
        for n in range(0, w_ref.shape[1], 256):
            cols.append(jnp.concatenate([jnp.dot(y_ref[t * sub + i * hs:t * sub + (i + 1) * hs, :], w_ref[:, n:n + 256], preferred_element_type=jnp.float32) for i in range(2)], axis=0))
        z = jnp.concatenate(cols, axis=1) + b_ref[...]
        for part, dst in ((0, q_ref), (1, k_ref)):
            for h in range(heads):
                x = z[:, part * d_local + h * HEAD:part * d_local + (h + 1) * HEAD]
                mean_sq = jnp.mean(x * x, axis=-1, keepdims=True)
                xn = x * lax.rsqrt(mean_sq + EPS) * gain_ref[part:part + 1, :]
                note(part * heads + h, jnp.max(jnp.sum(xn * xn, axis=-1, keepdims=True), axis=0, keepdims=True))
                rot = xn * cos_t + pltpu.roll(xn, HEAD // 2, 1) * sin_t
                dst[rows, h * HEAD:(h + 1) * HEAD] = rot.astype(jnp.bfloat16)
        v = z[:, 2 * d_local:3 * d_local]
        v_ref[rows, :] = v.astype(jnp.bfloat16)
        for h in range(heads):
            note(2 * heads + h, jnp.max(jnp.abs(v[:, h * HEAD:(h + 1) * HEAD]), axis=0, keepdims=True))
    n_ref[...] = jnp.zeros(n_ref.shape, jnp.float32)
    for i in range(3 * heads):
        n_ref[0, i:i + 1, :] = jnp.broadcast_to(stats[i], (1, HEAD))


def qkv_call(y, w, b, gains, hot, table, dl, rb=512, sub=512):
    n, d = y.shape
    d3 = w.shape[1]
    steps = n // rb
    row = lambda c: pl.BlockSpec((rb, c), lambda i: (i, 0))
    whole = lambda *s: pl.BlockSpec(s, lambda i: (0,) * len(s))
    return pl.pallas_call(
        functools.partial(qkv_kernel, sub=sub), grid=(steps,),
        in_specs=[row(d), whole(d, d3), whole(1, d3), whole(2, HEAD), row(hot.shape[1]), whole(*table.shape)],
        out_specs=[row(dl), row(dl), row(dl), pl.BlockSpec((1, 16, HEAD), lambda i: (i, 0, 0))],
        out_shape=[jax.ShapeDtypeStruct((n, dl), jnp.bfloat16)] * 3 + [jax.ShapeDtypeStruct((steps, 16, HEAD), jnp.float32)],
        compiler_params=pltpu.CompilerParams(vmem_limit_bytes=VMEM),
        cost_estimate=pl.CostEstimate(flops=2 * n * d * d3, bytes_accessed=2 * n * d + 2 * n * d3, transcendentals=0),
    )(y, w, b, gains, hot, table)


def attn_kernel(info_ref, q_ref, k_ref, v_ref, *refs, sub, bk):
    o_all, p_ref, vx_ref = refs[-3:]
    per = o_all.shape[2]
    h = pl.program_id(0)
    i = pl.program_id(1)
    n = k_ref.shape[0]
    bq = q_ref.shape[0]
    vid = n - TXT
    n_valid = info_ref[0]
    fast = info_ref[1 + h] == 1

    def tail_rows(width):
        return lax.broadcasted_iota(jnp.int32, (TXT, width), 0) + vid

    @pl.when(i == 0)
    def _():
        vx_ref[:, :HEAD] = v_ref[...]
        vx_ref[:vid, HEAD:] = jnp.ones((vid, HEAD), jnp.bfloat16)
        keep = jnp.where(tail_rows(HEAD) < n_valid, 1.0, 0.0).astype(jnp.bfloat16)
        vx_ref[vid:, HEAD:] = keep
        vx_ref[vid:, :HEAD] = jnp.where(tail_rows(HEAD) < n_valid, v_ref[vid:, :].astype(jnp.float32), 0.0).astype(jnp.bfloat16)

    @pl.when(fast)
    def _():
        def weighted(t):
            acc = jnp.dot(p_ref[t % 2], vx_ref[...], preferred_element_type=jnp.float32)
            o_all[t * sub // per, 0, t * sub % per:t * sub % per + sub, :] = (acc[:, :HEAD] / acc[:, HEAD:]).astype(jnp.bfloat16)

        for t in range(bq // sub):
            q = q_ref[t * sub:(t + 1) * sub, :]
            for j in range(n // bk):
                s = lax.dot_general(q, k_ref[j * bk:(j + 1) * bk, :], NT, preferred_element_type=jnp.float32)
                p_ref[t % 2, :, j * bk:(j + 1) * bk] = jnp.exp2(s * SCORE_EXP2).astype(jnp.bfloat16)
            if t > 0:
                weighted(t - 1)
        weighted(bq // sub - 1)

        @pl.when(i == n // bq - 1)
        def _():
            s = lax.dot_general(q_ref[bq - TXT:, :], k_ref[vid:, :], NT, preferred_element_type=jnp.float32)
            p = jnp.exp2(s * SCORE_EXP2).astype(jnp.bfloat16)
            pad = tail_rows(HEAD) >= n_valid
            vp = jnp.where(pad, v_ref[vid:, :].astype(jnp.float32), 0.0).astype(jnp.bfloat16)
            on = jnp.where(pad, 1.0, 0.0).astype(jnp.bfloat16)
            acc = jnp.dot(p, jnp.concatenate([vp, on], axis=1), preferred_element_type=jnp.float32)
            old = o_all[bq // per - 1, 0, per - TXT:, :].astype(jnp.float32)
            o_all[bq // per - 1, 0, per - TXT:, :] = jnp.where(pad, acc[:, :HEAD] / acc[:, HEAD:], old).astype(jnp.bfloat16)

    @pl.when(jnp.logical_not(fast))
    def _():
        bs = 256

        def rows(t, _):
            r0 = pl.multiple_of(t * bs, bs)
            q = q_ref[pl.ds(r0, bs), :]
            q_ok = (lax.broadcasted_iota(jnp.int32, (bs, bs), 0) + (i * bq + r0)) < n_valid

            def keys(j, carry):
                m, acc = carry
                c0 = pl.multiple_of(j * bs, bs)
                s = lax.dot_general(q, k_ref[pl.ds(c0, bs), :], NT, preferred_element_type=jnp.float32) * SCORE_EXP2
                k_ok = (lax.broadcasted_iota(jnp.int32, (bs, bs), 1) + c0) < n_valid
                s = jnp.where(q_ok == k_ok, s, -1e30)
                m_new = jnp.maximum(m, jnp.max(s, axis=1, keepdims=True))
                p = jnp.exp2(s - m_new).astype(jnp.bfloat16)
                vx = jnp.concatenate([v_ref[pl.ds(c0, bs), :], jnp.ones((bs, HEAD), jnp.bfloat16)], axis=1)
                return m_new, acc * jnp.exp2(m - m_new) + jnp.dot(p, vx, preferred_element_type=jnp.float32)

            m0 = jnp.full((bs, 1), -3e38, jnp.float32)
            _, acc = lax.fori_loop(0, n // bs, keys, (m0, jnp.zeros((bs, 2 * HEAD), jnp.float32)))
            o_all[lax.div(r0, per), 0, pl.ds(pl.multiple_of(lax.rem(r0, per), bs), bs), :] = (acc[:, :HEAD] / acc[:, HEAD:]).astype(jnp.bfloat16)
            return 0

        lax.fori_loop(0, bq // bs, rows, 0)


def attn_call(info, q, k, v, rows, slot, slots, out=None, bq=1024, sub=512, bk=1024):
    n, dl = q.shape
    heads = dl // HEAD
    kv = pl.BlockSpec((n, HEAD), lambda h, i, _: (0, h))
    args = [info, q, k, v] + ([] if out is None else [out])
    return pl.pallas_call(
        functools.partial(attn_kernel, sub=sub, bk=bk),
        grid_spec=pltpu.PrefetchScalarGridSpec(
            num_scalar_prefetch=1, grid=(heads, n // bq),
            in_specs=[pl.BlockSpec((bq, HEAD), lambda h, i, _: (i, h)), kv, kv] + [pl.BlockSpec(memory_space=pl.ANY)] * (len(args) - 4),
            out_specs=pl.BlockSpec((bq // rows, 1, rows, HEAD), lambda h, i, _: (i, slot, 0, h)),
            scratch_shapes=[pltpu.VMEM((2, sub, n), jnp.bfloat16), pltpu.VMEM((n, 2 * HEAD), jnp.bfloat16)]),
        out_shape=jax.ShapeDtypeStruct((n // rows, slots, rows, dl), jnp.bfloat16),
        input_output_aliases={} if out is None else {4: 0},
        compiler_params=pltpu.CompilerParams(vmem_limit_bytes=VMEM),
        cost_estimate=pl.CostEstimate(flops=8 * n * n * dl, bytes_accessed=8 * n * dl, transcendentals=n * n * heads),
    )(*args)


def mlp_kernel(*refs, ts, steps, n_stacks, first, proj, slots, final, aliased, nw):
    refs = list(refs)
    take = lambda k: [refs.pop(0) for _ in range(k)]
    n = len(ts)
    y_hbm = take(n if steps else 0)
    acc_hbm = take(0 if first else n)
    packs, bias = take(n_stacks), take(n_stacks)
    att_hbm = dict(zip(proj, take(len(proj))))
    oa_hbm, = take(1) if proj else (None,)
    tok_hbm, gate_ref, bout_ref = take(3) if final else (None,) * 3
    take(int(aliased))
    accs_out = [t for t in ts if t not in final]
    out_acc = dict(zip(accs_out, take(len(accs_out))))
    out_hbm, = take(1) if final else (None,)
    y_v, acc_v, w_v, u_v, h_v, bias_v, att_v, tok_v, y_sem, acc_sem, w_sem, out_sem, att_sem, tok_sem, tail_sem = refs
    tb, d_model = acc_v.shape[1:]
    _, _, group, width, _ = w_v.shape
    kdim = group * width
    n_steps = len(steps)
    chunk = 2 * kdim
    n_proj = d_model // chunk if proj else 0

    y_copy = lambda i: pltpu.make_async_copy(y_hbm[i], y_v.at[i], y_sem.at[i])
    acc_copy = lambda i: pltpu.make_async_copy(acc_hbm[i], acc_v.at[i], acc_sem.at[i])
    acc_store = lambda i: pltpu.make_async_copy(acc_v.at[i], out_acc[ts[i]], out_sem.at[i])
    out_rows = lambda i: pl.ds(ts[i] * tb, tb)
    tok_copy = lambda i: pltpu.make_async_copy(tok_hbm.at[out_rows(i), :], tok_v.at[final.index(ts[i])], tok_sem.at[final.index(ts[i])])
    out_store = lambda i: pltpu.make_async_copy(tok_v.at[final.index(ts[i])], out_hbm.at[out_rows(i), :], out_sem.at[i])

    def att_copies(j):
        att = att_hbm[proj[j]]
        w = att.shape[3]
        return [pltpu.make_async_copy(att.at[k, slots[j]], att_v.at[j, :, pl.ds(k * w, w)], att_sem.at[j, k]) for k in range(att.shape[0])]

    def weight_copies(s, slot, kind):
        if s >= n_steps:
            return [pltpu.make_async_copy(oa_hbm.at[s - n_steps, kind], w_v.at[slot, kind], w_sem.at[slot, kind, 0])]
        out, at = [], 0
        for k, (i, shard, b0, nb) in enumerate(steps[s]):
            out.append(pltpu.make_async_copy(packs[i].at[shard, kind, pl.ds(b0, nb)], w_v.at[slot, kind, pl.ds(at, nb)], w_sem.at[slot, kind, k]))
            at += nb
        return out

    def start_weights(s):
        for kind in range(2):
            for c in weight_copies(s, s % 2, kind):
                c.start()

    def arrive(s, slot):
        for kind in range(2):
            for c in weight_copies(s, slot, kind):
                c.wait()

    def follow(s, total, low):
        for k in range(low, total):
            @pl.when(s + 1 == k)
            def _():
                start_weights(k)

    def up(k, s, slot):
        t = lax.rem(k, n)
        for p in range(0, group, 2):
            w = w_v[slot, 0, p:p + 2].reshape(2 * width, d_model)
            at = slice(p * width, (p + 2) * width)
            u_v[:, at] = lax.dot_general(y_v[t], w, NT, preferred_element_type=jnp.float32) + bias_v[s, :, at]

    def act():
        u = u_v[...]
        half = 0.5 * u
        h_v[...] = (half * jnp.tanh(u * (GELU_1 * (u * u) + GELU_0)) + half).astype(jnp.bfloat16)

    def down(k, slot, store=False):
        t = n - 1 if store else lax.rem(k, n)
        for c in range(0, d_model, nw):
            w2 = w_v[slot, 1, :, :, c:c + nw].reshape(kdim, nw)
            old = acc_v[t, :, c:c + nw]
            if first:
                old = jnp.where(k < n, 0.0, old)
            acc_v[t, :, c:c + nw] = old + jnp.dot(h_v[...], w2, preferred_element_type=jnp.float32)
            if store:
                tail_store(c).start()

    def tail_store(c):
        at = pl.ds(c, nw)
        return pltpu.make_async_copy(acc_v.at[n - 1, :, at], out_acc[ts[n - 1]].at[:, at], tail_sem.at[c // nw])

    total = n_steps + n_proj
    if n_steps:
        for c in weight_copies(0, 0, 0):
            c.start()
        y_copy(0).start()
        for c in weight_copies(0, 0, 1):
            c.start()
    else:
        start_weights(0)
    for s, parts in enumerate(steps):
        at = 0
        for i, shard, b0, nb in parts:
            for b in range(b0, b0 + nb):
                bias_v[s, :, at * width:(at + 1) * width] = bias[i][shard, b:b + 1, :]
                at += 1
    if n_steps:
        for c in weight_copies(0, 0, 0):
            c.wait()
        y_copy(0).wait()
        for i in range(1, n):
            y_copy(i).start()
        if not first:
            acc_copy(0).start()
    for j in range(len(proj)):
        for c in att_copies(j):
            c.start()
    if not first:
        for i in range(int(bool(n_steps)), n):
            acc_copy(i).start()
    for t in final:
        tok_copy(ts.index(t)).start()
    if n_steps:
        up(0, 0, 0)
        for c in weight_copies(0, 0, 1):
            c.wait()
        last = n * n_steps - 1

        def trip(k, _):
            s = lax.div(k, n)
            before = lax.div(k - 1, n)
            for i in range(1, n):
                @pl.when(k == i)
                def _():
                    y_copy(i).wait()
            if not first:
                for i in range(n):
                    @pl.when(k - 1 == i)
                    def _():
                        acc_copy(i).wait()
            if n_steps > 1:
                @pl.when((lax.rem(k, n) == 0) & (k > 0))
                def _():
                    arrive(0, lax.rem(s, 2))
            if total > 1:
                @pl.when(lax.rem(k, n) == 1)
                def _():
                    follow(s, total, 1)
            if not proj:
                for i in range(n - 2):
                    @pl.when(k - 2 - (last + 1 - n) == i)
                    def _():
                        acc_store(i).start()
            act()
            up(k, s, lax.rem(s, 2))
            down(k - 1, lax.rem(before, 2))
            return 0

        lax.fori_loop(1, last + 1, trip, 0)
        if not proj and n > 1:
            acc_store(n - 2).start()
        act()
        if not first and n_steps == 1:
            acc_copy(n - 1).wait()
        down(last, (n_steps - 1) % 2, store=not proj)
    elif not first:
        for i in range(n):
            acc_copy(i).wait()
    if proj:
        for i, t in enumerate(ts):
            if t not in proj:
                acc_store(i).start()
        for j in range(len(proj)):
            for c in att_copies(j):
                c.wait()
        base = ts.index(proj[0])

        def turn(k, _, closing=False):
            c = lax.div(k, len(proj)) if not closing else n_proj - 1
            j = lax.rem(k, len(proj)) if not closing else k
            slot = lax.rem(n_steps + c, 2)
            if not closing:
                @pl.when(j == 0)
                def _():
                    arrive(n_steps, slot)
                    follow(n_steps + c, total, n_steps + 1)
            elif j == 0:
                arrive(n_steps, slot)
            t = proj[j] if closing else None
            last = closing and t in final
            if last:
                tok_copy(base + j).wait()
            at = c * chunk if closing else pl.multiple_of(c * chunk, chunk)
            h = att_v[j, :, pl.ds(at, chunk)]
            for e in range(0, d_model, nw):
                w2 = w_v[slot, :, :, :, e:e + nw].reshape(chunk, nw)
                part = acc_v[base + j, :, e:e + nw] + jnp.dot(h, w2, preferred_element_type=jnp.float32)
                if last:
                    f = final.index(t)
                    res = tok_v[f, :, e:e + nw].astype(jnp.float32) + gate_ref[t:t + 1, e:e + nw] * (part + bout_ref[:, e:e + nw])
                    tok_v[f, :, e:e + nw] = res.astype(jnp.bfloat16)
                else:
                    acc_v[base + j, :, e:e + nw] = part
            if closing:
                (out_store if last else acc_store)(base + j).start()
            return 0

        lax.fori_loop(0, (n_proj - 1) * len(proj), turn, 0)
        for j in range(len(proj)):
            turn(j, 0, closing=True)
    for i, t in enumerate(ts):
        if i == n - 1 and not proj:
            for c in range(0, d_model, nw):
                tail_store(c).wait()
        else:
            (out_store if t in final else acc_store)(i).wait()


def mlp_call(ts, y, acc, stacks, steps, proj=(), att=(), w_oa=None, final=(), tail=None, group=4, nw=512):
    tb, d = (y or acc)[0].shape
    n = len(ts)
    first = acc is None
    width = 128
    hbm = pl.BlockSpec(memory_space=pl.ANY)
    vm = pl.BlockSpec(memory_space=pltpu.VMEM)
    args, specs = [], []

    def add(spec, *xs):
        args.extend(xs)
        specs.extend([spec] * len(xs))

    if steps:
        add(hbm, *y)
    if not first:
        add(hbm, *acc)
    add(hbm, *[s[0] for s in stacks])
    add(vm, *[s[1] for s in stacks])
    add(hbm, *[a for a, _ in att])
    if proj:
        add(hbm, w_oa.reshape(d // (2 * group * width), 2, group, width, d))
    alias = {}
    n_acc = n - len(final)
    outs = [jax.ShapeDtypeStruct((tb, d), jnp.float32)] * n_acc
    if final:
        tokens, gate, b_out, out = tail
        add(hbm, tokens)
        add(vm, gate, b_out)
        if out is not None:
            add(hbm, out)
            alias = {len(args) - 1: n_acc}
        outs.append(jax.ShapeDtypeStruct(tokens.shape, tokens.dtype))
    n_steps = len(steps)
    n_par = max(1, len(proj))
    has = lambda c, *s: s if c else (8, 128)
    scratch = [
        pltpu.VMEM(has(n_steps, n, tb, d), jnp.bfloat16), pltpu.VMEM((n, tb, d), jnp.float32),
        pltpu.VMEM((2, 2, group, width, d), jnp.bfloat16),
        pltpu.VMEM(has(n_steps, tb, group * width), jnp.float32), pltpu.VMEM(has(n_steps, tb, group * width), jnp.bfloat16),
        pltpu.VMEM((max(1, n_steps), 1, group * width), jnp.float32),
        pltpu.VMEM(has(proj, n_par, tb, d), jnp.bfloat16), pltpu.VMEM(has(final, max(1, len(final)), tb, d), jnp.bfloat16),
        pltpu.SemaphoreType.DMA((n,)), pltpu.SemaphoreType.DMA((n,)), pltpu.SemaphoreType.DMA((2, 2, group)), pltpu.SemaphoreType.DMA((n,)),
        pltpu.SemaphoreType.DMA((n_par, 8)), pltpu.SemaphoreType.DMA((max(1, len(final)),)), pltpu.SemaphoreType.DMA((d // nw,))]
    cols = n_steps * group * width
    rows = n * tb
    res = pl.pallas_call(
        functools.partial(mlp_kernel, ts=tuple(ts), steps=steps, n_stacks=len(stacks), first=first, proj=tuple(proj), slots=tuple(slot for _, slot in att), final=tuple(final), aliased=bool(alias), nw=nw),
        in_specs=specs, out_specs=[hbm] * len(outs), out_shape=outs, input_output_aliases=alias, scratch_shapes=scratch,
        compiler_params=pltpu.CompilerParams(vmem_limit_bytes=VMEM),
        cost_estimate=pl.CostEstimate(flops=4 * rows * d * cols + 2 * len(proj) * tb * d * d, bytes_accessed=4 * d * cols + 10 * rows * d, transcendentals=rows * cols),
    )(*args)
    return (list(res[:n_acc]), res[n_acc]) if final else (list(res), None)


def pick_kernel(where_ref, src_hbm, dst_hbm, buf, in_sem, out_sem):
    n = dst_hbm.shape[0]
    todo = [(i, j) for i in range(n) for j in range(dst_hbm.shape[1])]
    load = lambda i, j: pltpu.make_async_copy(src_hbm.at[where_ref[i], j], buf.at[i, j], in_sem.at[i, j])
    store = lambda i, j: pltpu.make_async_copy(buf.at[i, j], dst_hbm.at[i, j], out_sem.at[i, j])
    for ij in todo:
        load(*ij).start()
    for ij in todo:
        load(*ij).wait()
        store(*ij).start()
    for ij in todo:
        store(*ij).wait()


def pick_call(where, a):
    shape = (where.shape[0],) + a.shape[1:]
    hbm = pl.BlockSpec(memory_space=pl.ANY)
    return pl.pallas_call(
        pick_kernel,
        grid_spec=pltpu.PrefetchScalarGridSpec(
            num_scalar_prefetch=1, grid=(1,), in_specs=[hbm], out_specs=hbm,
            scratch_shapes=[pltpu.VMEM(shape, a.dtype), pltpu.SemaphoreType.DMA(shape[:2]), pltpu.SemaphoreType.DMA(shape[:2])]),
        out_shape=jax.ShapeDtypeStruct(shape, a.dtype),
        compiler_params=pltpu.CompilerParams(vmem_limit_bytes=VMEM),
        cost_estimate=pl.CostEstimate(flops=4 * math.prod(shape), bytes_accessed=4 * math.prod(shape), transcendentals=0),
    )(where, a)


def pack_kernel(first_ref, in_ref, out_ref, o_ref):
    o_ref[0, 0] = in_ref[...].T
    o_ref[1, 0] = out_ref[...]


def pack_call(first, count, w_in, w_out, width):
    d = w_in.shape[0]
    return pl.pallas_call(
        pack_kernel,
        grid_spec=pltpu.PrefetchScalarGridSpec(
            num_scalar_prefetch=1, grid=(count,),
            in_specs=[pl.BlockSpec((d, width), lambda i, f: (0, f[0] + i)), pl.BlockSpec((width, d), lambda i, f: (f[0] + i, 0))],
            out_specs=pl.BlockSpec((2, 1, width, d), lambda i, f: (0, i, 0, 0))),
        out_shape=jax.ShapeDtypeStruct((2, count, width, d), w_in.dtype),
        cost_estimate=pl.CostEstimate(flops=4 * count * width * d, bytes_accessed=8 * count * width * d, transcendentals=0),
    )(first[None], w_in, w_out)


def mod_kernel(me_ref, c_ref, w_ref, o_ref):
    @pl.when(pl.program_id(0) == 0)
    def _():
        o_ref[...] = jnp.zeros(o_ref.shape, jnp.float32)

    o_ref[...] += jnp.dot(c_ref[...], w_ref[...], preferred_element_type=jnp.float32)


def mod_call(me, cond, w, cols, kb=768):
    b, d = cond.shape
    return pl.pallas_call(
        mod_kernel,
        grid_spec=pltpu.PrefetchScalarGridSpec(
            num_scalar_prefetch=1, grid=(d // kb,),
            in_specs=[pl.BlockSpec((b, kb), lambda i, m: (0, i)), pl.BlockSpec((kb, cols), lambda i, m: (i, m[0]))],
            out_specs=pl.BlockSpec((b, cols), lambda i, m: (0, 0))),
        out_shape=jax.ShapeDtypeStruct((b, cols), jnp.float32),
        cost_estimate=pl.CostEstimate(flops=2 * b * d * cols, bytes_accessed=2 * d * cols, transcendentals=0),
    )(me[None], cond, w)


def order_kernel(w_ref, hot_ref, o_ref):
    d_local = w_ref.shape[2]
    for c in range(2):
        for h in range(d_local // HEAD):
            at = slice(h * HEAD, (h + 1) * HEAD)
            o_ref[:, c * d_local + h * HEAD:c * d_local + (h + 1) * HEAD] = jnp.dot(
                w_ref[c, :, at], hot_ref[...], preferred_element_type=jnp.float32).astype(o_ref.dtype)
    o_ref[:, 2 * d_local:3 * d_local] = w_ref[2]
    o_ref[:, 3 * d_local:] = jnp.zeros((o_ref.shape[0], o_ref.shape[1] - 3 * d_local), o_ref.dtype)


def order_call(w, hot, rb=512):
    _, d, d_local = w.shape
    cols = -(-3 * d_local // 256) * 256
    return pl.pallas_call(
        order_kernel, grid=(d // rb,),
        in_specs=[pl.BlockSpec((3, rb, d_local), lambda i: (0, i, 0)), pl.BlockSpec((HEAD, HEAD), lambda i: (0, 0))],
        out_specs=pl.BlockSpec((rb, cols), lambda i: (i, 0)),
        out_shape=jax.ShapeDtypeStruct((d, cols), w.dtype),
        cost_estimate=pl.CostEstimate(flops=4 * d * d_local * HEAD, bytes_accessed=12 * d * d_local, transcendentals=0),
    )(w, hot)


def rope_rows(grid_hw, seq_len, sizes):
    tok_idx = jnp.arange(seq_len, dtype=jnp.int32)
    grid_h, grid_w = grid_hw[0], grid_hw[1]
    video = (tok_idx < seq_len - TXT).astype(jnp.int32)
    pos = (tok_idx // (grid_h * grid_w), (tok_idx // grid_w) % grid_h, tok_idx % grid_w)
    lane = jnp.arange(2 * HEAD, dtype=jnp.int32)[None, :]
    hit, start = None, 0
    for p, size in zip(pos, sizes):
        here = lane == (p * video + start)[:, None]
        hit = here if hit is None else hit | here
        start += size
    return hit.astype(jnp.bfloat16)


def rope_table(sizes):
    pair_idx = jnp.arange(HEAD // 2, dtype=jnp.int32)
    axis_sel = (pair_idx >= 8).astype(jnp.int32) + (pair_idx >= 36).astype(jnp.int32)
    within = pair_idx - jnp.where(axis_sel == 0, 0, jnp.where(axis_sel == 1, 8, 36))
    inv_freq = jnp.power(THETA, -2.0 * within.astype(jnp.float32) / jnp.where(axis_sel == 0, 16.0, 56.0))
    row = jnp.arange(2 * HEAD, dtype=jnp.int32)[:, None]
    start, table = 0, jnp.zeros((2 * HEAD, 2 * HEAD), jnp.float32)
    for axis, size in enumerate(sizes):
        angles = (row - start).astype(jnp.float32) * inv_freq
        cos_t, sin_t = jnp.cos(angles), jnp.sin(angles)
        live = (row >= start) & (row < start + size) & (jnp.tile(axis_sel, 4)[None, :] == axis)
        table = jnp.where(live, jnp.concatenate([cos_t, cos_t, -sin_t, sin_t], axis=1), table)
        start += size
    top = table.astype(jnp.bfloat16)
    rest = table - top.astype(jnp.float32)
    mid = rest.astype(jnp.bfloat16)
    low = (rest - mid.astype(jnp.float32)).astype(jnp.bfloat16)
    return jnp.concatenate([top, mid, low], axis=1)


def modulated_norm(tokens, shift, scale):
    tok_f32 = tokens.astype(jnp.float32)
    centered = tok_f32 - jnp.mean(tok_f32, axis=-1, keepdims=True)
    variance = jnp.mean(centered * centered, axis=-1, keepdims=True)
    normed = centered * lax.rsqrt(variance + EPS)
    return (normed * (1.0 + scale) + shift).astype(jnp.bfloat16)


def split_pairs(x):
    s = x.shape
    return jnp.swapaxes(x.reshape(s[:-1] + (s[-1] // HEAD, HEAD // 2, 2)), -1, -2).reshape(s)


def solution(mesh):
    n_tp, n_dp = mesh.shape['tp'], mesh.shape['dp']
    n_x = n_tp // 2
    twin = [(i, i ^ 1) for i in range(n_dp)]
    core = [(i, i ^ 1) for i in range(n_tp)]

    def block_step(tokens, cond_vec, txt_len, grid_hw, w_mod, b_mod, w_qkv, b_qkv, q_gain, k_gain, w_mlp_in, b_mlp_in, w_out_attn, w_out_mlp, b_out):
        batch, rows, d_model = tokens.shape
        seq = rows * n_tp
        d_local = w_qkv.shape[2]
        heads = d_local // HEAD
        width = 128
        n_blk = w_mlp_in.shape[1] // width
        half = n_blk // 2
        side = lax.axis_index('dp') % 2
        me = lax.axis_index('tp')
        cpos, xpos = me % 2, me // 2

        def after(x, *deps):
            return lax.optimization_barrier((x,) + deps)[0]

        def gather(a, tiled=False):
            return lax.all_gather(a, 'tp', axis=0, tiled=tiled)

        def gather_small(a):
            a, step = a[None], 1
            while step < n_tp:
                b = lax.ppermute(a, 'tp', [(i, i ^ step) for i in range(n_tp)])
                a = jnp.where((me // step) % 2 == 0, jnp.concatenate([a, b]), jnp.concatenate([b, a]))
                step *= 2
            return a

        swap = lambda a: lax.ppermute(a, 'tp', core)
        cross = lambda a: lax.ppermute(a, 'dp', twin)
        mine = side * half
        theirs = half - mine
        chunks = ((0, 2), (2, 2), (4, 2))
        pack = lambda first, count, *deps: pack_call(after(first, *deps), count, w_mlp_in, w_out_mlp, width)
        packs = [pack(mine, chunks[0][1])]

        n_mod = w_mod.shape[1] // n_tp
        mod_part = mod_call(after(me, packs[0]), jax.nn.silu(cond_vec).astype(jnp.bfloat16), w_mod, n_mod)
        small = gather_small(jnp.concatenate([mod_part.reshape(-1), b_mlp_in]))
        own_pack = pack(theirs, half, mod_part)[None]
        mate_pack = swap(own_pack)
        for b0, nb in chunks[1:]:
            packs.append(pack(mine + b0, nb, own_pack))
        mod_all = jnp.swapaxes(small[:, :batch * n_mod].reshape(n_tp, batch, n_mod), 0, 1).reshape(batch, -1) + b_mod
        shift, scale, gate = mod_all[:, :d_model], mod_all[:, d_model:2 * d_model], mod_all[:, 2 * d_model:]
        bias = small[:, batch * n_mod:].reshape(n_tp, n_blk, width)
        bias_g = lax.dynamic_slice_in_dim(bias, mine, half, 1)
        bias_n = lax.dynamic_slice_in_dim(bias, theirs, half, 1)
        y_own = [modulated_norm(tokens[s], shift[s], scale[s]) for s in range(batch)]
        y_full = [gather(y_own[s], tiled=True) for s in range(batch)]
        l_pack = [gather(packs[i]) for i in range(len(chunks))]

        w_oa = gather(w_out_attn, tiled=True)
        far_ids = jnp.stack([2 * ((xpos + j) % n_x) + cpos for j in range(1, n_x)])
        near_ids = [2 * ((xpos + j) % n_x) + 1 - cpos for j in range(1, n_x)]
        perm = jnp.arange(HEAD)
        perm = (perm % (HEAD // 2)) * 2 + perm // (HEAD // 2)
        one_hot = (jnp.arange(HEAD)[:, None] == perm[None, :]).astype(jnp.bfloat16)
        w_all = order_call(jnp.swapaxes(w_qkv, 0, 1), one_hot)
        b_all = jnp.concatenate([split_pairs(b_qkv[:2]).reshape(-1), b_qkv[2], jnp.zeros((w_all.shape[1] - 3 * d_local,), jnp.float32)])[None]
        gains = split_pairs(jnp.stack([q_gain, k_gain]))
        sizes = (16, 96, 96)
        table = rope_table(sizes)
        hots = [rope_rows(grid_hw[s], seq, sizes) for s in range(batch)]

        own = (own_pack, lax.dynamic_index_in_dim(bias_n, me, 0))
        mate = (mate_pack, lax.dynamic_index_in_dim(bias_n, me ^ 1, 0))
        left, far, near, qkv, att, spread = {}, {}, {}, {}, {}, {}
        place = {0: (0, 2), 1: (1, 2), 2: (0, 1)}
        state = {'last': None, 'acc': None, 'out': None}

        def turn(x):
            return x if state['last'] is None else after(x, state['last'])

        def do_send(i):
            b0, nb = chunks[i]
            left[i] = (l_pack[i], bias_g[:, b0:b0 + nb])
            state['last'] = pick_call(far_ids, turn(l_pack[i]))
            d_pack = cross(state['last'])
            far[i] = (d_pack, jnp.stack([bias_n[2 * ((xpos + j) % n_x) + cpos, b0:b0 + nb] for j in range(1, n_x)]))

        def do_relay(i):
            b0, nb = chunks[i]
            e_pack = swap(turn(far[i][0]))
            near[i] = (e_pack, jnp.stack([bias_n[j, b0:b0 + nb] for j in near_ids]))

        def do_qkv(s):
            qkv[s] = qkv_call(turn(y_full[s]), w_all, b_all, gains, hots[s], table, d_local)
            state['last'] = qkv[s][0]

        def do_attend(s):
            q, k, v, stats = qkv[s]
            top = jnp.max(stats, axis=(0, 2))
            bound = jnp.sqrt(top[:heads] * top[heads:2 * heads]) * (SCORE_EXP2 * 1.02) + 1.0
            v_top = top[2 * heads:3 * heads]
            fast = (bound < 100.0) & (v_top * jnp.exp2(bound) < 2.0 ** 110)
            info = jnp.concatenate([(seq - TXT + txt_len[s])[None], fast.astype(jnp.int32)])
            att[s] = attn_call(info, turn(q), k, v, rows, *place[s], out=att[s - 1] if place[s][0] else None)
            state['last'] = att[s]

        def do_spread(samples):
            moved = lax.all_to_all(turn(att[samples[-1]]), 'tp', 0, 0, tiled=False)
            for s in samples:
                spread[s] = (moved, place[s][0])

        def do_mlp(names, proj=(), final=(), ts=tuple(range(batch))):
            stacks, flat = [], []
            for name in names:
                i = int(name[1:] or 0)
                for stack in {'O': (own, mate), 'L': (left.get(i),), 'D': (far.get(i), near.get(i))}[name[0]]:
                    stacks.append(stack)
                    n_shards, _, nb = stack[0].shape[:3]
                    flat += [(len(stacks) - 1, j, b, 1) for j in range(n_shards) for b in range(nb)]
            steps = [flat[i:i + 4] for i in range(0, len(flat), 4)]
            y = [y_own[t] for t in ts]
            acc = state['acc'] and [state['acc'][t] for t in ts]
            if acc:
                acc[0] = turn(acc[0])
            elif steps:
                y[0] = turn(y[0])
            tail = (tokens.reshape(batch * rows, d_model), gate, b_out[None], state['out'])
            accs, out = mlp_call(ts, y, acc, stacks, steps, proj=proj, att=[spread[t] for t in proj], w_oa=w_oa, final=final, tail=tail)
            left_over = [t for t in ts if t not in final]
            state['acc'] = {**(state['acc'] or {}), **dict(zip(left_over, accs))}
            if out is not None:
                state['out'] = out
            state['last'] = (accs + [out])[0]

        do_mlp(['O'])
        state['last'] = after(state['last'], w_all, *hots)
        do_send(0)
        do_mlp(['L0'])
        do_qkv(0)
        do_attend(0)
        do_relay(0)
        do_send(1)
        do_mlp(['L1', 'D0'])
        do_qkv(1)
        do_attend(1)
        do_relay(1)
        do_send(2)
        do_mlp(['L2', 'D1'])
        do_qkv(2)
        do_spread((0, 1))
        do_attend(2)
        do_relay(2)
        do_mlp(['D2'])
        do_spread((2,))
        do_mlp([], proj=(0, 1), final=(0, 1), ts=(0, 1))
        do_mlp([], proj=(2,), final=(2,), ts=(2,))
        return state['out'].reshape(batch, rows, d_model)

    in_specs = (P('dp', 'tp', None), P('dp', None), P('dp'), P('dp', None), P(None, None), P(None), P(None, None, 'tp'), P(None, 'tp'), P(None), P(None), P(None, 'tp'), P('tp'), P('tp', None), P('tp', None), P(None))
    return jax.shard_map(block_step, mesh=mesh, in_specs=in_specs, out_specs=P('dp', 'tp', None), check_vma=False)
```
